32 devices in a mesh: dp: 4 (over z), tp: 8 (over y, x, core).
Axes of the slice: x: 2, y: 2, z: 4, core: 2. Of those that a mesh axis runs over, the one named last changes fastest.
Arguments:
- x_in: bfloat16 [4, 2048, 2048], P('dp', 'tp'), parts along dimension 0
- cond_vec: bfloat16 [4, 2048], P('dp'), parts along dimension 0
- rope_cos: float32 [2048, 64], P('tp')
- rope_sin: float32 [2048, 64], P('tp')
- w_mod: bfloat16 [2, 2048, 6144], replicated
- b_mod: bfloat16 [2, 6144], replicated
- w_in: bfloat16 [2, 2048, 16, 896], P(None, None, 'tp')
- b_in: bfloat16 [2, 16, 896], P(None, 'tp')
- q_scale: bfloat16 [2, 128], replicated
- k_scale: bfloat16 [2, 128], replicated
- w_out: bfloat16 [2, 16, 640, 2048], P(None, 'tp')
- b_out: bfloat16 [2, 2048], replicated
- d_out: bfloat16 [4, 2048, 2048], P('dp', 'tp'), parts along dimension 0
Outputs:
- output 1: bfloat16 [4, 2048, 2048], P('dp', 'tp'), parts along dimension 0
- output 2: bfloat16 [4, 2048, 2048], P('dp', 'tp'), parts along dimension 0
- output 3: float32 [8, 2048, 6144], P('dp'), parts along dimension 0
- output 4: float32 [8, 6144], P('dp'), parts along dimension 0
- output 5: bfloat16 [8, 2048, 16, 896], P('dp', None, 'tp'), parts along dimension 0
- output 6: float32 [8, 16, 896], P('dp', 'tp'), parts along dimension 0
- output 7: float32 [8, 128], P('dp'), parts along dimension 0
- output 8: float32 [8, 128], P('dp'), parts along dimension 0
- output 9: bfloat16 [8, 16, 640, 2048], P('dp', 'tp'), parts along dimension 0
- output 10: float32 [8, 2048], P('dp'), parts along dimension 0
There are 4 independent parts. The reference program is written for one: setup_inputs(seed, part) draws one part's arguments, and reference() takes and returns one part's arrays. A program takes and returns all parts, laid end to end along the dimension named above; an argument that names none is the same for every part.
All inputs are finite; a program needn't handle non-finite values.
Results may differ from the reference program's by a relative error of at most 0.02.
Values are sent between devices in bfloat16 or wider.
A program may use at most 1 GiB of HBM per device.

```python
import jax
import jax.numpy as jnp
from jax import lax

MODEL_DIM = 2048
NUM_HEADS = 16
HEAD_DIM = 128
MLP_DIM = 8192
SEQ_LEN = 2048
BATCH_SIZE = 1
NUM_BLOCKS = 2

GROUP_MLP = MLP_DIM // NUM_HEADS
GROUP_COLS = 3 * HEAD_DIM + GROUP_MLP
GROUP_ROWS = HEAD_DIM + GROUP_MLP
TEXT_LEN = SEQ_LEN // 4
HALF_DIM = HEAD_DIM // 2
NORM_EPS = 1e-6


def rope_tables(table_key):
    key_w, key_r, key_c = jax.random.split(table_key, 3)
    grid_width = jax.random.randint(key_w, (), 8, 65)
    row_off = jax.random.randint(key_r, (), 0, 32)
    col_off = jax.random.randint(key_c, (), 0, 32)
    token_idx = jnp.arange(SEQ_LEN) - TEXT_LEN
    is_image = token_idx >= 0
    safe_idx = jnp.maximum(token_idx, 0)
    row_pos = jnp.where(is_image, safe_idx // grid_width + row_off, 0).astype(jnp.float32)
    col_pos = jnp.where(is_image, safe_idx % grid_width + col_off, 0).astype(jnp.float32)
    n_zero = HALF_DIM // 8
    n_row = (HALF_DIM - n_zero) // 2
    n_col = HALF_DIM - n_zero - n_row
    freq_row = 10000.0 ** (-jnp.arange(n_row, dtype=jnp.float32) / n_row)
    freq_col = 10000.0 ** (-jnp.arange(n_col, dtype=jnp.float32) / n_col)
    angles = jnp.concatenate([jnp.zeros((SEQ_LEN, n_zero), jnp.float32), row_pos[:, None] * freq_row[None, :], col_pos[:, None] * freq_col[None, :]], axis=1)
    return jnp.cos(angles), jnp.sin(angles)


def setup_inputs(seed: int = 0, part: int = 0) -> dict:
    base_key = jax.random.key(seed)
    shared_keys = jax.random.split(base_key, 12)
    own_keys = jax.random.split(jax.random.fold_in(base_key, part), 4)
    is_text = (jnp.arange(SEQ_LEN) < TEXT_LEN)[None, :, None]
    x_raw = jax.random.normal(own_keys[0], (BATCH_SIZE, SEQ_LEN, MODEL_DIM), jnp.float32)
    text_shift = 0.8 * jax.random.normal(own_keys[1], (MODEL_DIM,), jnp.float32)
    x_in = jnp.where(is_text, 0.6 * x_raw + text_shift, x_raw)
    cond_vec = jax.random.normal(own_keys[2], (BATCH_SIZE, MODEL_DIM), jnp.float32)
    d_out = jax.random.normal(own_keys[3], (BATCH_SIZE, SEQ_LEN, MODEL_DIM), jnp.float32)
    rope_cos, rope_sin = rope_tables(shared_keys[0])
    w_mod = jax.random.normal(shared_keys[1], (NUM_BLOCKS, MODEL_DIM, 3 * MODEL_DIM), jnp.float32) * MODEL_DIM ** -0.5
    b_mod = 0.5 * jax.random.normal(shared_keys[2], (NUM_BLOCKS, 3 * MODEL_DIM), jnp.float32)
    w_in = jax.random.normal(shared_keys[3], (NUM_BLOCKS, MODEL_DIM, NUM_HEADS, GROUP_COLS), jnp.float32) * MODEL_DIM ** -0.5
    b_in = 0.3 * jax.random.normal(shared_keys[4], (NUM_BLOCKS, NUM_HEADS, GROUP_COLS), jnp.float32)
    q_scale = 1.5 + 0.4 * jax.random.normal(shared_keys[5], (NUM_BLOCKS, HEAD_DIM), jnp.float32)
    k_scale = 1.5 + 0.4 * jax.random.normal(shared_keys[6], (NUM_BLOCKS, HEAD_DIM), jnp.float32)
    w_out = jax.random.normal(shared_keys[7], (NUM_BLOCKS, NUM_HEADS, GROUP_ROWS, MODEL_DIM), jnp.float32) * (MODEL_DIM + MLP_DIM) ** -0.5
    b_out = 0.3 * jax.random.normal(shared_keys[8], (NUM_BLOCKS, MODEL_DIM), jnp.float32)
    return {"x_in": x_in.astype(jnp.bfloat16), "cond_vec": cond_vec.astype(jnp.bfloat16), "rope_cos": rope_cos, "rope_sin": rope_sin, "w_mod": w_mod.astype(jnp.bfloat16), "b_mod": b_mod.astype(jnp.bfloat16), "w_in": w_in.astype(jnp.bfloat16), "b_in": b_in.astype(jnp.bfloat16), "q_scale": q_scale.astype(jnp.bfloat16), "k_scale": k_scale.astype(jnp.bfloat16), "w_out": w_out.astype(jnp.bfloat16), "b_out": b_out.astype(jnp.bfloat16), "d_out": d_out.astype(jnp.bfloat16)}


def to_bf16(tensor):
    return tensor.astype(jnp.bfloat16).astype(jnp.float32)


def rms_norm(tensor):
    return tensor * lax.rsqrt(jnp.mean(tensor * tensor, axis=-1, keepdims=True) + NORM_EPS)


def layer_norm(tensor):
    row_mean = jnp.mean(tensor, axis=-1, keepdims=True)
    centered = tensor - row_mean
    row_var = jnp.mean(centered * centered, axis=-1, keepdims=True)
    return centered * lax.rsqrt(row_var + NORM_EPS)


def apply_rope(tensor, rope_cos, rope_sin):
    pair_view = tensor.reshape(tensor.shape[:-1] + (tensor.shape[-1] // 2, 2))
    even_part = pair_view[..., 0]
    odd_part = pair_view[..., 1]
    cos_wide = rope_cos[None, :, None, :]
    sin_wide = rope_sin[None, :, None, :]
    rotated = jnp.stack([even_part * cos_wide - odd_part * sin_wide, even_part * sin_wide + odd_part * cos_wide], axis=-1)
    return rotated.reshape(tensor.shape)


def head_attention(operands):
    q_head, k_head, v_head = operands
    scores = jnp.einsum("bqe,bke->bqk", q_head, k_head) * (HEAD_DIM ** -0.5)
    attn_probs = jax.nn.softmax(scores, axis=-1)
    return to_bf16(jnp.einsum("bqk,bke->bqe", to_bf16(attn_probs), v_head))


def block_forward(x_f32, silu_vec, rope_cos, rope_sin, layer_params):
    w_mod, b_mod, w_in, b_in, q_scale, k_scale, w_out, b_out = layer_params
    mod_vec = jnp.dot(silu_vec, w_mod, preferred_element_type=jnp.float32) + b_mod
    mod_shift, mod_scale, mod_gate = jnp.split(mod_vec, 3, axis=-1)
    normed = to_bf16(layer_norm(x_f32) * (1.0 + mod_scale[:, None, :]) + mod_shift[:, None, :])
    projected = jnp.einsum("bsd,dhc->bshc", normed, w_in) + b_in
    q_rot = to_bf16(apply_rope(rms_norm(projected[..., :HEAD_DIM]) * q_scale, rope_cos, rope_sin))
    k_rot = to_bf16(apply_rope(rms_norm(projected[..., HEAD_DIM:2 * HEAD_DIM]) * k_scale, rope_cos, rope_sin))
    v_part = to_bf16(projected[..., 2 * HEAD_DIM:3 * HEAD_DIM])
    mlp_act = to_bf16(jax.nn.gelu(projected[..., 3 * HEAD_DIM:], approximate=True))
    per_head = lax.map(jax.checkpoint(head_attention), (jnp.moveaxis(q_rot, 2, 0), jnp.moveaxis(k_rot, 2, 0), jnp.moveaxis(v_part, 2, 0)))
    attn_out = jnp.moveaxis(per_head, 0, 2)
    joined = jnp.concatenate([attn_out, mlp_act], axis=-1)
    mixed_out = jnp.einsum("bshc,hcd->bsd", joined, w_out)
    return to_bf16(x_f32 + mod_gate[:, None, :] * (mixed_out + b_out))


def reference(x_in, cond_vec, rope_cos, rope_sin, w_mod, b_mod, w_in, b_in, q_scale, k_scale, w_out, b_out, d_out):
    silu_vec = to_bf16(jax.nn.silu(cond_vec.astype(jnp.float32)))
    weights = tuple(weight.astype(jnp.float32) for weight in (w_mod, b_mod, w_in, b_in, q_scale, k_scale, w_out, b_out))

    def stack_forward(x_f32, all_params):
        def layer_step(state_in, layer_params):
            return block_forward(state_in, silu_vec, rope_cos, rope_sin, layer_params), None
        final_state, unused = lax.scan(layer_step, x_f32, all_params)
        return final_state

    out_f32, pullback = jax.vjp(stack_forward, x_in.astype(jnp.float32), weights)
    grad_x, grad_w = pullback(d_out.astype(jnp.float32))
    return (out_f32.astype(jnp.bfloat16), grad_x.astype(jnp.bfloat16), grad_w[0], grad_w[1], grad_w[2].astype(jnp.bfloat16), grad_w[3], grad_w[4], grad_w[5], grad_w[6].astype(jnp.bfloat16), grad_w[7])
```

```python
import functools
import jax
import jax.numpy as jnp
from jax import lax
from jax.experimental import pallas as pl
from jax.experimental.pallas import tpu as pltpu
from jax.sharding import PartitionSpec as P

EPS = 1e-6
MESH = pl.DeviceIdType.MESH
ANY = pl.BlockSpec(memory_space=pl.ANY)
VM = pl.BlockSpec(memory_space=pltpu.VMEM)
F32 = jnp.float32
BF16 = jnp.bfloat16
LOG2E = 1.4426950408889634
VMEM_LIMIT = 62 * 1024 * 1024


def dot(a, b, dims=((1,), (0,)), precision=None):
    return lax.dot_general(a, b, (dims, ((), ())), preferred_element_type=F32, precision=precision)


def neighbours():
    me = lax.axis_index("tp")
    core = lax.rem(me, 2)
    xbit = lax.rem(lax.div(me, 2), 2)
    ybit = lax.div(me, 4)
    return {"p": me + 1 - 2 * core, "x": me + 2 - 4 * xbit, "y": me + 4 - 8 * ybit}


def slot_owner(slot):
    me = lax.axis_index("tp")
    out = me
    for bit in range(3):
        if (slot >> bit) & 1:
            mine = lax.rem(lax.div(me, 1 << bit), 2)
            out = out + (1 << bit) - (2 << bit) * mine
    return out


def barrier(nbrs):
    sem = pltpu.get_barrier_semaphore()
    for key in ("p", "x", "y"):
        pl.semaphore_signal(sem, inc=1, device_id={"tp": nbrs[key]}, device_id_type=MESH)
    pl.semaphore_wait(sem, 3)


class Gather:
    def __init__(self, buf, send, recv, nbrs, chunks):
        self.buf, self.send, self.recv, self.nbrs, self.chunks = buf, send, recv, nbrs, chunks
        self.rows = buf.shape[1] // chunks
        self.index = {}
        for ch in range(chunks):
            for key in (("y", 0, 4), ("x", 0, 2), ("p", 0, 1), ("p", 2, 3), ("p", 4, 5), ("p", 6, 7)):
                self.index[key + (ch,)] = len(self.index)
            key = ("y", 2, 6) if self.via_x(ch) else ("x", 4, 6)
            self.index[key + (ch,)] = len(self.index)

    def via_x(self, ch):
        return ch < (self.chunks + 1) // 2

    def copy(self, to, src, dst, ch):
        rows = pl.ds(ch * self.rows, self.rows)
        return pltpu.make_async_remote_copy(
            src_ref=self.buf.at[src, rows],
            dst_ref=self.buf.at[dst, rows],
            send_sem=self.send.at[self.index[(to, src, dst, ch)]],
            recv_sem=self.recv.at[dst * self.chunks + ch],
            device_id={"tp": self.nbrs[to]},
            device_id_type=MESH,
        )

    def start_own(self):
        for ch in range(self.chunks):
            self.copy("y", 0, 4, ch).start()
            self.copy("x", 0, 2, ch).start()
        for ch in range(self.chunks):
            self.copy("p", 0, 1, ch).start()

    def arrived(self, slot, ch):
        to, src = {1: ("p", 0), 2: ("x", 0), 3: ("p", 2), 4: ("y", 0), 5: ("p", 4), 7: ("p", 6)}.get(slot, (None, None))
        if slot == 6:
            to, src = ("y", 2) if self.via_x(ch) else ("x", 4)
        self.copy(to, src, slot, ch).wait_recv()

    def wait_slot(self, slot):
        for ch in range(self.chunks):
            self.arrived(slot, ch)

    def pass_neighbours(self):
        order = []
        half = (self.chunks + 1) // 2
        for ch in range(self.chunks):
            order.append((2, ch))
            order.append((4, ch))
        for slot, ch in order:
            self.arrived(slot, ch)
            if slot == 2 and self.via_x(ch):
                self.copy("y", 2, 6, ch).start()
            if slot == 4 and not self.via_x(ch):
                self.copy("x", 4, 6, ch).start()
            self.copy("p", slot, slot + 1, ch).start()

    def pass_diagonal(self):
        half = (self.chunks + 1) // 2
        for k in range(half):
            for ch in (k, k + half):
                if ch < self.chunks:
                    self.arrived(6, ch)
                    self.copy("p", 6, 7, ch).start()

    def before(self, step):
        @pl.when(step == 1)
        def _():
            self.wait_slot(1)

        @pl.when(step == 2)
        def _():
            self.pass_neighbours()

        @pl.when(step == 3)
        def _():
            self.wait_slot(3)

        @pl.when(step == 5)
        def _():
            self.wait_slot(5)

        @pl.when(step == 6)
        def _():
            self.pass_diagonal()

        @pl.when(step == 7)
        def _():
            self.wait_slot(7)

    def all_now(self):
        self.start_own()
        self.pass_neighbours()
        self.pass_diagonal()
        for slot in (1, 3, 5, 7):
            self.wait_slot(slot)

    def finish(self):
        for key in self.index:
            self.copy(*key).wait_send()


def gather_sems(chunks):
    return [pltpu.SemaphoreType.DMA((7 * chunks,)), pltpu.SemaphoreType.DMA((8 * chunks,))]


class Reduce:
    SENDS = ("p3", "p2", "p1", "p0", "xd", "yd", "yb", "ya", "xa", "xb")

    def __init__(self, part, pout, pin, dsum, ysum, xsum, xin, yin, ownx, owny, ykeep, xkeep, send, recv, nbrs):
        self.part, self.pout, self.pin = part, pout, pin
        self.dsum, self.ysum, self.xsum = dsum, ysum, xsum
        self.xin, self.yin, self.ownx, self.owny = xin, yin, ownx, owny
        self.ykeep, self.xkeep = ykeep, xkeep
        self.send, self.recv, self.nbrs = send, recv, nbrs
        self.half = part.shape[0] // 2

    def copy(self, key):
        lo, hi = pl.ds(0, self.half), pl.ds(self.half, self.half)
        src, dst, to = {
            "p3": (self.pout.at[3], self.pin.at[3], "p"),
            "p2": (self.pout.at[2], self.pin.at[2], "p"),
            "p1": (self.pout.at[1], self.pin.at[1], "p"),
            "p0": (self.pout.at[0], self.pin.at[0], "p"),
            "xd": (self.dsum.at[lo], self.xin, "x"),
            "yd": (self.dsum.at[hi], self.yin, "y"),
            "yb": (self.ysum.at[hi], self.owny.at[hi], "y"),
            "ya": (self.ysum.at[lo], self.owny.at[lo], "y"),
            "xa": (self.xsum.at[lo], self.ownx.at[lo], "x"),
            "xb": (self.xsum.at[hi], self.ownx.at[hi], "x"),
        }[key]
        i = self.SENDS.index(key)
        return pltpu.make_async_remote_copy(
            src_ref=src, dst_ref=dst, send_sem=self.send.at[i], recv_sem=self.recv.at[i],
            device_id={"tp": self.nbrs[to]}, device_id_type=MESH,
        )

    def rows_loop(self, start, count, body, step=16):
        def one(i, carry):
            body(pl.ds(pl.multiple_of(start + i * step, step), step), pl.ds(pl.multiple_of(i * step, step), step))
            return carry
        lax.fori_loop(0, count // step, one, 0)

    def after(self, step):
        half, full = self.half, 2 * self.half
        part, pin = self.part, self.pin

        for z in (3, 2, 1, 0):
            @pl.when(step == 6 - 2 * z)
            def _(z=z):
                def body(rows, unused):
                    self.pout[z, rows, :] = part[rows, :].astype(BF16)
                self.rows_loop(0, full, body)
                self.copy(f"p{z}").start()

        @pl.when(step == 1)
        def _():
            self.copy("p3").wait_recv()
            def body(rows, unused):
                self.dsum[rows, :] = (part[rows, :] + pin[3, rows, :].astype(F32)).astype(BF16)
            self.rows_loop(0, half, body)
            self.copy("xd").start()
            self.rows_loop(half, half, body)
            self.copy("yd").start()

        @pl.when(step == 3)
        def _():
            self.copy("p2").wait_recv()
            def body(rows, unused):
                self.ysum[rows, :] = (part[rows, :] + pin[2, rows, :].astype(F32)).astype(BF16)
            self.rows_loop(half, half, body)
            self.copy("yb").start()
            def keep(rows, base):
                self.ykeep[base, :] = part[rows, :] + pin[2, rows, :].astype(F32)
            self.rows_loop(0, half, keep)

        @pl.when(step == 5)
        def _():
            self.copy("p1").wait_recv()
            def body(rows, unused):
                self.xsum[rows, :] = (part[rows, :] + pin[1, rows, :].astype(F32)).astype(BF16)
            self.rows_loop(0, half, body)
            self.copy("xa").start()
            def keep(rows, base):
                self.xkeep[base, :] = part[rows, :] + pin[1, rows, :].astype(F32)
            self.rows_loop(half, half, keep)

    def relay_y(self):
        self.copy("xd").wait_recv()
        def body(rows, base):
            self.ysum[rows, :] = (self.ykeep[base, :] + self.xin[base, :].astype(F32)).astype(BF16)
        self.rows_loop(0, self.half, body)
        self.copy("ya").start()

    def relay_x(self):
        self.copy("yd").wait_recv()
        def body(rows, base):
            self.xsum[rows, :] = (self.xkeep[base, :] + self.yin[base, :].astype(F32)).astype(BF16)
        self.rows_loop(self.half, self.half, body)
        self.copy("xb").start()

    def wait_own(self):
        for key in ("p0", "xa", "yb", "ya", "xb"):
            self.copy(key).wait_recv()

    def own(self, rows):
        return (self.part[rows, :] + self.pin[0, rows, :].astype(F32)) + (
            self.ownx[rows, :].astype(F32) + self.owny[rows, :].astype(F32))

    def finish(self):
        for key in self.SENDS:
            self.copy(key).wait_send()


def reduce_scratch(tok, dim):
    half = tok // 2
    return [
        pltpu.VMEM((tok, dim), F32),
        pltpu.VMEM((4, tok, dim), BF16),
        pltpu.VMEM((4, tok, dim), BF16),
        pltpu.VMEM((tok, dim), BF16),
        pltpu.VMEM((tok, dim), BF16),
        pltpu.VMEM((tok, dim), BF16),
        pltpu.VMEM((half, dim), BF16),
        pltpu.VMEM((half, dim), BF16),
        pltpu.VMEM((tok, dim), BF16),
        pltpu.VMEM((tok, dim), BF16),
        pltpu.VMEM((half, dim), F32),
        pltpu.VMEM((half, dim), F32),
        pltpu.SemaphoreType.DMA((10,)),
        pltpu.SemaphoreType.DMA((10,)),
    ]


def comm_params(cid):
    return pltpu.CompilerParams(collective_id=cid, has_side_effects=True, vmem_limit_bytes=VMEM_LIMIT)


def prologue_kernel(cond, cos, sin, b_mod, w_mod, mod_out, cosx_out, sinx_out,
                    wbuf, wsem, mbuf, rbuf, ms, mr, rs, rr):
    nbrs = neighbours()
    me = lax.axis_index("tp")
    blocks, dim, cols = wbuf.shape
    tok, half = cos.shape
    mine = pl.ds(pl.multiple_of(me * cols, cols), cols)
    loads = [pltpu.make_async_copy(w_mod.at[b, :, mine], wbuf.at[b], wsem.at[b]) for b in range(blocks)]
    for load in loads:
        load.start()
    rbuf[0, :, :half] = cos[...]
    rbuf[0, :, half:] = sin[...]
    vec = cond[...].astype(F32)
    silu = (vec * jax.nn.sigmoid(vec)).astype(BF16)
    barrier(nbrs)
    rope = Gather(rbuf, rs, rr, nbrs, 2)
    rope.start_own()
    for b in range(blocks):
        loads[b].wait()
        mbuf[0, b:b + 1, :] = dot(silu, wbuf[b]) + b_mod[b:b + 1, mine].astype(F32)
    mods = Gather(mbuf, ms, mr, nbrs, 1)
    mods.start_own()
    mods.pass_neighbours()
    rope.pass_neighbours()
    mods.pass_diagonal()
    rope.pass_diagonal()
    for slot in (1, 3, 5, 7):
        mods.wait_slot(slot)
        rope.wait_slot(slot)
    for slot in range(8):
        owner = slot_owner(slot)
        mod_out[:, pl.ds(pl.multiple_of(owner * cols, cols), cols)] = mbuf[slot]
    row = lax.broadcasted_iota(jnp.int32, (2 * half, 2 * half), 0)
    lane = lax.broadcasted_iota(jnp.int32, (2 * half, 2 * half), 1)
    pick_cos = jnp.where(row == lax.div(lane, 2), 1.0, 0.0).astype(F32)
    sign = jnp.where(lax.rem(lane, 2) == 0, -1.0, 1.0)
    pick_sin = jnp.where(row == half + lax.div(lane, 2), sign, 0.0).astype(F32)

    def expand(slot, carry):
        both = rbuf[slot]
        cosx_out[slot] = dot(both, pick_cos, precision=lax.Precision.HIGHEST)
        sinx_out[slot] = dot(both, pick_sin, precision=lax.Precision.HIGHEST)
        return carry
    lax.fori_loop(0, 8, expand, 0)
    mods.finish()
    rope.finish()


def prologue(cond, cos, sin, b_mod, w_mod):
    tok, half = cos.shape
    blocks, dim, width = w_mod.shape
    cols = width // 8
    return pl.pallas_call(
        prologue_kernel,
        out_shape=[jax.ShapeDtypeStruct((blocks, width), F32)] + [jax.ShapeDtypeStruct((8, tok, 2 * half), F32)] * 2,
        in_specs=[VM] * 4 + [ANY],
        out_specs=[VM] * 3,
        scratch_shapes=[pltpu.VMEM((blocks, dim, cols), BF16), pltpu.SemaphoreType.DMA((blocks,)),
                        pltpu.VMEM((8, blocks, cols), F32), pltpu.VMEM((8, tok, 2 * half), F32)]
        + gather_sems(1) + gather_sems(2),
        compiler_params=comm_params(0),
        name="prologue",
    )(cond, cos, sin, b_mod, w_mod)


def swap_pairs(tensor):
    lane = lax.broadcasted_iota(jnp.int32, tensor.shape, 1)
    size = tensor.shape[1]
    return jnp.where(lax.rem(lane, 2) == 0, pltpu.roll(tensor, size - 1, 1), pltpu.roll(tensor, 1, 1))


GELU_C = 0.7978845608028654
GELU_A = 0.044715


def gelu(u):
    return 0.5 * u * (1.0 + jnp.tanh(GELU_C * (u + GELU_A * (u * u * u))))


def gelu_grad(u):
    square = u * u
    t = jnp.tanh(GELU_C * (u + GELU_A * (square * u)))
    inner = GELU_C * (1.0 + 3.0 * GELU_A * square)
    return 0.5 * (1.0 + t) + 0.5 * u * (1.0 - t * t) * inner


def layer_norm_rows(x):
    mean = jnp.mean(x, axis=-1, keepdims=True)
    centered = x - mean
    var = jnp.mean(centered * centered, axis=-1, keepdims=True)
    rstd = lax.rsqrt(var + EPS)
    return centered * rstd, rstd


def fwd_in_kernel(blk, x, mod, b_in, qs, ks, cosx, sinx, w_in,
                  h_out, q_out, k_out, v_out, pre_out, u_out, m_out, w_out,
                  hbuf, wraw, wbuf, proj, qst, kst, vst, pst, ust, mst, wsem, osem, hsem, wosem, gs, gr):
    nbrs = neighbours()
    _, tok, dim = hbuf.shape
    cols = b_in.shape[2]
    hd = qs.shape[1]
    loads = dim // 512 if dim >= 512 else 1
    per = dim // loads
    def wload(i):
        rows = pl.ds(i * per, per)
        return pltpu.make_async_copy(w_in.at[blk, rows], wraw.at[rows], wsem.at[i])
    for i in range(loads):
        wload(i).start()
    shift = mod[blk:blk + 1, :dim]
    scale1 = 1.0 + mod[blk:blk + 1, dim:2 * dim]
    def norm(i, carry):
        rows = pl.ds(pl.multiple_of(i * 16, 16), 16)
        normed, _ = layer_norm_rows(x[rows, :].astype(F32))
        hbuf[0, rows, :] = (normed * scale1 + shift).astype(BF16)
        return carry
    lax.fori_loop(0, tok // 16, norm, 0)
    barrier(nbrs)
    gather = Gather(hbuf, gs, gr, nbrs, 4)
    gather.start_own()

    row = lax.broadcasted_iota(jnp.int32, (256, 256), 0)
    lane = lax.broadcasted_iota(jnp.int32, (256, 256), 1)
    pick = jnp.where(lane == 2 * lax.rem(row, 128) + lax.div(row, 128), 1.0, 0.0).astype(BF16)
    for i in range(loads):
        wload(i).wait()
        def split(t, carry, i=i):
            base = pl.multiple_of(i * per + t * 128, 128)
            both = wraw[pl.ds(base, 128)].reshape(256, cols)
            apart = dot(pick, both).astype(BF16)
            wbuf[pl.ds(base, 128), :cols] = apart[:128]
            wbuf[pl.ds(base, 128), cols:] = apart[128:]
            return carry
        lax.fori_loop(0, per // 128, split, 0)
    pltpu.make_async_copy(wbuf, w_out, wosem).start()

    def stores(step, slot):
        return [pltpu.make_async_copy(src.at[slot], dst.at[step], osem.at[slot, j])
                for j, (src, dst) in enumerate(((qst, q_out), (kst, k_out), (vst, v_out), (pst, pre_out), (ust, u_out), (mst, m_out)))]

    def body(step, carry):
        gather.before(step)
        par = lax.rem(step, 2)
        pltpu.make_async_copy(hbuf.at[step], h_out.at[step], hsem.at[step]).start()
        @pl.when(step >= 2)
        def _():
            for cp in stores(step - 2, par):
                cp.wait()
        proj[...] = dot(hbuf[step], wbuf[...])
        def epilogue(i, carry):
            rows = pl.ds(pl.multiple_of(i * 32, 32), 32)
            cx, sx = cosx[step, rows, :], sinx[step, rows, :]
            for head in range(2):
                base = head * cols
                bias = b_in[blk, head:head + 1, :].astype(F32)
                here = pl.ds(head * hd, hd)
                for which, (gain, dst) in enumerate(((qs, qst), (ks, kst))):
                    lanes = which * hd
                    t = proj[rows, base + lanes:base + lanes + hd] + bias[:, lanes:lanes + hd]
                    pst[par, rows, (2 * which + head) * hd:(2 * which + head + 1) * hd] = t
                    n = t * lax.rsqrt(jnp.mean(t * t, axis=-1, keepdims=True) + EPS)
                    n = n * gain[blk:blk + 1, :].astype(F32)
                    dst[par, rows, here] = (n * cx + swap_pairs(n) * sx).astype(BF16)
                vst[par, rows, here] = (proj[rows, base + 2 * hd:base + 3 * hd] + bias[:, 2 * hd:3 * hd]).astype(BF16)
                mlp = cols - 3 * hd
                for j in range(mlp // 128):
                    lo = 3 * hd + j * 128
                    u = proj[rows, base + lo:base + lo + 128] + bias[:, lo:lo + 128]
                    ust[par, rows, head * mlp + j * 128:head * mlp + j * 128 + 128] = u
                    mst[par, rows, head * mlp + j * 128:head * mlp + j * 128 + 128] = gelu(u).astype(BF16)
            return carry
        lax.fori_loop(0, tok // 32, epilogue, 0)
        for cp in stores(step, par):
            cp.start()
        return carry
    lax.fori_loop(0, 8, body, 0)
    for step in (6, 7):
        for cp in stores(step, step % 2):
            cp.wait()
    for step in range(8):
        pltpu.make_async_copy(hbuf.at[step], h_out.at[step], hsem.at[step]).wait()
    pltpu.make_async_copy(wbuf, w_out, wosem).wait()
    gather.finish()


def fwd_in(blk, x, mod, b_in, qs, ks, cosx, sinx, w_in):
    tok, dim = x.shape
    cols = w_in.shape[3]
    hd = qs.shape[1]
    mlp = cols - 3 * hd
    s = jax.ShapeDtypeStruct
    loads = dim // 512 if dim >= 512 else 1
    return pl.pallas_call(
        functools.partial(fwd_in_kernel, blk),
        out_shape=[s((8, tok, dim), BF16)] + [s((8, tok, 2 * hd), BF16)] * 3
        + [s((8, tok, 4 * hd), F32), s((8, tok, 2 * mlp), F32), s((8, tok, 2 * mlp), BF16), s((dim, 2 * cols), BF16)],
        in_specs=[VM] * 7 + [ANY],
        out_specs=[ANY] * 8,
        scratch_shapes=[pltpu.VMEM((8, tok, dim), BF16), pltpu.VMEM((dim, 2, cols), BF16), pltpu.VMEM((dim, 2 * cols), BF16),
                        pltpu.VMEM((tok, 2 * cols), F32)]
        + [pltpu.VMEM((2, tok, 2 * hd), BF16)] * 3
        + [pltpu.VMEM((2, tok, 4 * hd), F32), pltpu.VMEM((2, tok, 2 * mlp), F32), pltpu.VMEM((2, tok, 2 * mlp), BF16)]
        + [pltpu.SemaphoreType.DMA((loads,)), pltpu.SemaphoreType.DMA((2, 6)), pltpu.SemaphoreType.DMA((8,)),
           pltpu.SemaphoreType.DMA] + gather_sems(4),
        compiler_params=comm_params(1 + blk),
        name=f"fwd_in{blk}",
    )(x, mod, b_in, qs, ks, cosx, sinx, w_in)


def fwd_out_kernel(blk, x, mod, b_out, k, v, q, m, w_out, x_new, branch_out, o_out, of_out, lse_out,
                   wbuf, sc, pn, ost, ofst, lst, wsem, osem, *red):
    nbrs = neighbours()
    tok, dim = x.shape
    hd = k.shape[2] // 2
    seq = 8 * tok
    mlp = m.shape[2] // 2
    c2 = LOG2E * hd ** -0.5
    load = pltpu.make_async_copy(w_out.at[blk], wbuf, wsem)
    load.start()
    barrier(nbrs)
    rs = Reduce(*red, nbrs)
    load.wait()

    def stores(slot, par):
        return [pltpu.make_async_copy(src.at[par], dst.at[slot], osem.at[par, j])
                for j, (src, dst) in enumerate(((ost, o_out), (ofst, of_out), (lst, lse_out)))]

    def body(step, carry):
        slot = 7 - step
        par = lax.rem(step, 2)
        @pl.when(step >= 2)
        def _():
            for cp in stores(slot + 2, par):
                cp.wait()
        for head in range(2):
            here = pl.ds(head * hd, hd)
            qh = q[slot, :, here]
            kh = k[:, :, here].reshape(seq, hd)
            sc[...] = dot(qh, kh, ((1,), (1,)))
            vh = v[:, :, here].reshape(seq, hd)
            def soft(i, carry):
                rows = pl.ds(pl.multiple_of(i * 32, 32), 32)
                top = jnp.max(sc[rows, :], axis=-1, keepdims=True) * c2
                e = jnp.exp2(sc[rows, :] * c2 - top)
                total = jnp.sum(e, axis=-1, keepdims=True)
                pn[rows, :] = (e * (1.0 / total)).astype(BF16)
                lst[par, head, rows, :] = jnp.broadcast_to(top + jnp.log2(total), (32, 128))
                return carry
            lax.fori_loop(0, tok // 32, soft, 0)
            o = dot(pn[...], vh)
            ofst[par, :, here] = o
            ost[par, :, here] = o.astype(BF16)
        acc = None
        part = red[0]
        nb = dim // 512 if dim >= 512 else 1
        wd = dim // nb
        for n in range(nb):
            lanes = pl.ds(n * wd, wd)
            acc = None
            for head in range(2):
                t = dot(ost[par, :, head * hd:(head + 1) * hd], wbuf[head, :hd, lanes])
                t = t + dot(m[slot, :, head * mlp:(head + 1) * mlp], wbuf[head, hd:, lanes])
                acc = t if acc is None else acc + t
            part[:, lanes] = acc
        for cp in stores(slot, par):
            cp.start()
        rs.after(step)
        @pl.when(step == 4)
        def _():
            rs.relay_y()
        @pl.when(step == 5)
        def _():
            rs.relay_x()
        return carry
    lax.fori_loop(0, 8, body, 0)
    for slot in (1, 0):
        for cp in stores(slot, (7 - slot) % 2):
            cp.wait()
    rs.wait_own()
    gate = mod[blk:blk + 1, 2 * dim:]
    bias = b_out[blk:blk + 1, :].astype(F32)
    def final(i, carry):
        rows = pl.ds(pl.multiple_of(i * 16, 16), 16)
        branch = rs.own(rows) + bias
        branch_out[rows, :] = branch
        x_new[rows, :] = (x[rows, :].astype(F32) + gate * branch).astype(BF16)
        return carry
    lax.fori_loop(0, tok // 16, final, 0)
    rs.finish()


def fwd_out(blk, x, mod, b_out, k, v, q, m, w_out):
    tok, dim = x.shape
    hd = k.shape[2] // 2
    s = jax.ShapeDtypeStruct
    return pl.pallas_call(
        functools.partial(fwd_out_kernel, blk),
        out_shape=[s((tok, dim), BF16), s((tok, dim), F32), s((8, tok, 2 * hd), BF16), s((8, tok, 2 * hd), F32),
                   s((8, 2, tok, 128), F32)],
        in_specs=[VM] * 7 + [ANY],
        out_specs=[VM] * 2 + [ANY] * 3,
        scratch_shapes=[pltpu.VMEM(w_out.shape[1:], BF16), pltpu.VMEM((tok, 8 * tok), F32), pltpu.VMEM((tok, 8 * tok), BF16),
                        pltpu.VMEM((2, tok, 2 * hd), BF16), pltpu.VMEM((2, tok, 2 * hd), F32), pltpu.VMEM((2, 2, tok, 128), F32),
                        pltpu.SemaphoreType.DMA, pltpu.SemaphoreType.DMA((2, 3))] + reduce_scratch(tok, dim),
        compiler_params=comm_params(3 + blk),
        name=f"fwd_out{blk}",
    )(x, mod, b_out, k, v, q, m, w_out)


def bwd_out_kernel(blk, grad, branch, mod, qs, ks, k, v, q, cosx, sinx, of, lse, pre, u, w_out,
                   db_out, dproj_out, g_bin, d_gate, d_bout, d_qs, d_ks,
                   dbuf, wbuf, dj, dk, dv, dqs, pt, dst, dpst, dkst, ofb, lseb, preb, ub, wsem, isem, osem, ksem, dsem, gs, gr):
    nbrs = neighbours()
    _, tok, dim = dbuf.shape
    hd = qs.shape[1]
    seq = 8 * tok
    mlp = u.shape[2] // 2
    cols = 3 * hd + mlp
    c2 = LOG2E * hd ** -0.5
    load = pltpu.make_async_copy(w_out.at[blk], wbuf, wsem)
    load.start()
    gate = mod[blk:blk + 1, 2 * dim:]

    def fetch(step, par):
        return [pltpu.make_async_copy(src.at[step], dstb.at[par], isem.at[par, j])
                for j, (src, dstb) in enumerate(((of, ofb), (lse, lseb), (pre, preb), (u, ub)))]

    for cp in fetch(0, 0):
        cp.start()

    def head_of(i, carry):
        dgate, dbias = carry
        rows = pl.ds(pl.multiple_of(i * 16, 16), 16)
        g = grad[rows, :].astype(F32)
        gated = g * gate
        dbuf[0, rows, :] = gated.astype(BF16)
        prod = g * branch[rows, :]
        return dgate + prod[:8] + prod[8:], dbias + gated[:8] + gated[8:]
    zero = jnp.zeros((8, dim), F32)
    dgate, dbias = lax.fori_loop(0, tok // 16, head_of, (zero, zero))
    barrier(nbrs)
    gather = Gather(dbuf, gs, gr, nbrs, 4)
    gather.start_own()
    d_gate[...] = jnp.sum(dgate, axis=0, keepdims=True)
    d_bout[...] = jnp.sum(dbias, axis=0, keepdims=True)
    g_bin[...] = jnp.zeros(g_bin.shape, F32)
    d_qs[...] = jnp.zeros(d_qs.shape, F32)
    d_ks[...] = jnp.zeros(d_ks.shape, F32)
    dk[...] = jnp.zeros(dk.shape, F32)
    dv[...] = jnp.zeros(dv.shape, F32)
    load.wait()

    def norm_rope_back(t, dy, cx, sx, gain):
        d = dy * cx - swap_pairs(dy) * sx
        r = lax.rsqrt(jnp.mean(t * t, axis=-1, keepdims=True) + EPS)
        n = t * r
        dn = d * gain
        return r * (dn - n * jnp.mean(dn * n, axis=-1, keepdims=True)), d * n

    def store(step, par):
        return [pltpu.make_async_copy(dpst.at[par], dproj_out.at[step], osem.at[par])]

    def body(step, carry):
        gather.before(step)
        par = lax.rem(step, 2)
        pltpu.make_async_copy(dbuf.at[step], db_out.at[step], dsem.at[step]).start()
        @pl.when(step < 7)
        def _():
            for cp in fetch(step + 1, 1 - par):
                cp.start()
        for head in range(2):
            dj[:, head * (hd + mlp):(head + 1) * (hd + mlp)] = dot(dbuf[step], wbuf[head], ((1,), (1,))).astype(BF16)
        for cp in fetch(step, par):
            cp.wait()
        @pl.when(step >= 2)
        def _():
            for cp in store(step - 2, par):
                cp.wait()
        for head in range(2):
            here = pl.ds(head * hd, hd)
            joined0 = head * (hd + mlp)
            do = dj[:, joined0:joined0 + hd]
            qh = q[step, :, here]
            delta = jnp.sum(jnp.transpose(do.astype(F32) * ofb[par, :, here]), axis=0, keepdims=True)
            lrow = jnp.transpose(lseb[par, head])[:1, :]
            def keys(j, carry):
                kh = k[j, :, here]
                vh = v[j, :, here]
                st = dot(kh, qh, ((1,), (1,)))
                p = jnp.exp2(st * c2 - lrow)
                dp = dot(vh, do, ((1,), (1,)))
                ds = (p * (dp - delta)).astype(BF16)
                dv[j, :, here] += dot(p.astype(BF16), do)
                dk[j, :, here] += dot(ds, qh)
                dst[pl.ds(pl.multiple_of(j * tok, tok), tok), :] = ds
                return carry
            lax.fori_loop(0, 8, keys, 0, unroll=2)
            kh = k[:, :, here].reshape(seq, hd)
            dqs[:, here] = dot(dst[...], kh, ((0,), (0,))) * (hd ** -0.5)

        def epilogue(i, carry):
            rows = pl.ds(pl.multiple_of(i * 32, 32), 32)
            cx, sx = cosx[step, rows, :], sinx[step, rows, :]
            for head in range(2):
                base = head * cols
                t = preb[par, rows, head * hd:(head + 1) * hd]
                gain = qs[blk:blk + 1, :].astype(F32)
                dy = dqs[rows, head * hd:(head + 1) * hd].astype(BF16).astype(F32)
                dt, dg = norm_rope_back(t, dy, cx, sx, gain)
                d_qs[...] += jnp.sum(dg, axis=0, keepdims=True)
                g_bin[:, base:base + hd] += jnp.sum(dt, axis=0, keepdims=True)
                dpst[par, rows, base:base + hd] = dt.astype(BF16)
                dkst[step, rows, head * hd:(head + 1) * hd] = preb[par, rows, (2 + head) * hd:(3 + head) * hd]
                for j in range(mlp // 128):
                    lo = j * 128
                    dm = dj[rows, head * (hd + mlp) + hd + lo:head * (hd + mlp) + hd + lo + 128].astype(F32)
                    du = dm * gelu_grad(ub[par, rows, head * mlp + lo:head * mlp + lo + 128])
                    g_bin[:, base + 3 * hd + lo:base + 3 * hd + lo + 128] += jnp.sum(du, axis=0, keepdims=True)
                    dpst[par, rows, base + 3 * hd + lo:base + 3 * hd + lo + 128] = du.astype(BF16)
            return carry
        lax.fori_loop(0, tok // 32, epilogue, 0)
        for cp in store(step, par):
            cp.start()
        return carry
    lax.fori_loop(0, 8, body, 0)
    for step in (6, 7):
        for cp in store(step, step % 2):
            cp.wait()

    def tail_copies(step, par):
        return [pltpu.make_async_copy(pt.at[par, :, pl.ds(head * 2 * hd, 2 * hd)],
                                      dproj_out.at[step, :, pl.ds(head * cols + hd, 2 * hd)], ksem.at[par, head]) for head in range(2)]

    def tail(step, carry):
        par = lax.rem(step, 2)
        @pl.when(step >= 2)
        def _():
            for cp in tail_copies(step - 2, par):
                cp.wait()
        def rows_of(i, carry):
            rows = pl.ds(pl.multiple_of(i * 32, 32), 32)
            cx, sx = cosx[step, rows, :], sinx[step, rows, :]
            for head in range(2):
                here = slice(head * hd, (head + 1) * hd)
                base = head * cols
                dy = (dk[step, rows, here] * (hd ** -0.5)).astype(BF16).astype(F32)
                dt, dg = norm_rope_back(dkst[step, rows, here], dy, cx, sx, ks[blk:blk + 1, :].astype(F32))
                d_ks[...] += jnp.sum(dg, axis=0, keepdims=True)
                g_bin[:, base + hd:base + 2 * hd] += jnp.sum(dt, axis=0, keepdims=True)
                pt[par, rows, head * 2 * hd:head * 2 * hd + hd] = dt.astype(BF16)
                dvr = dv[step, rows, here].astype(BF16)
                g_bin[:, base + 2 * hd:base + 3 * hd] += jnp.sum(dvr.astype(F32), axis=0, keepdims=True)
                pt[par, rows, head * 2 * hd + hd:(head + 1) * 2 * hd] = dvr
            return carry
        lax.fori_loop(0, tok // 32, rows_of, 0)
        for cp in tail_copies(step, par):
            cp.start()
        return carry
    lax.fori_loop(0, 8, tail, 0)
    for step in (6, 7):
        for cp in tail_copies(step, step % 2):
            cp.wait()
    for step in range(8):
        pltpu.make_async_copy(dbuf.at[step], db_out.at[step], dsem.at[step]).wait()
    gather.finish()


def bwd_out(blk, grad, branch, mod, qs, ks, k, v, q, cosx, sinx, of, lse, pre, u, w_out):
    tok, dim = grad.shape
    hd = qs.shape[1]
    mlp = u.shape[2] // 2
    cols = 3 * hd + mlp
    s = jax.ShapeDtypeStruct
    return pl.pallas_call(
        functools.partial(bwd_out_kernel, blk),
        out_shape=[s((8, tok, dim), BF16), s((8, tok, 2 * cols), BF16), s((1, 2 * cols), F32), s((1, dim), F32), s((1, dim), F32),
                   s((1, hd), F32), s((1, hd), F32)],
        in_specs=[VM] * 10 + [ANY] * 5,
        out_specs=[ANY] * 2 + [VM] * 5,
        scratch_shapes=[pltpu.VMEM((8, tok, dim), BF16), pltpu.VMEM(w_out.shape[1:], BF16), pltpu.VMEM((tok, 2 * (hd + mlp)), BF16),
                        pltpu.VMEM((8, tok, 2 * hd), F32), pltpu.VMEM((8, tok, 2 * hd), F32), pltpu.VMEM((tok, 2 * hd), F32),
                        pltpu.VMEM((2, tok, 4 * hd), BF16), pltpu.VMEM((8 * tok, tok), BF16), pltpu.VMEM((2, tok, 2 * cols), BF16),
                        pltpu.VMEM((8, tok, 2 * hd), F32),
                        pltpu.VMEM((2, tok, 2 * hd), F32), pltpu.VMEM((2, 2, tok, 128), F32), pltpu.VMEM((2, tok, 4 * hd), F32),
                        pltpu.VMEM((2, tok, 2 * mlp), F32),
                        pltpu.SemaphoreType.DMA, pltpu.SemaphoreType.DMA((2, 4)), pltpu.SemaphoreType.DMA((2,)),
                        pltpu.SemaphoreType.DMA((2, 2)), pltpu.SemaphoreType.DMA((8,))] + gather_sems(4),
        compiler_params=comm_params(5 + blk),
        name=f"bwd_out{blk}",
    )(grad, branch, mod, qs, ks, k, v, q, cosx, sinx, of, lse, pre, u, w_out)


def bwd_in_kernel(blk, grad, x, mod, dproj, w, g_new, d_shift, d_scale, wbuf, dbuf, wsem, dsem, *red):
    nbrs = neighbours()
    tok, dim = x.shape
    load = pltpu.make_async_copy(w, wbuf, wsem)
    load.start()
    def fetch(step):
        return pltpu.make_async_copy(dproj.at[7 - step], dbuf.at[step], dsem.at[step])
    for step in range(8):
        fetch(step).start()
    barrier(nbrs)
    rs = Reduce(*red, nbrs)
    load.wait()
    part = red[0]

    def body(step, carry):
        fetch(step).wait()
        part[...] = dot(dbuf[step], wbuf[...], ((1,), (1,)))
        rs.after(step)
        return carry
    lax.fori_loop(0, 8, body, 0)
    rs.relay_y()
    rs.relay_x()
    rs.wait_own()
    scale1 = 1.0 + mod[blk:blk + 1, dim:2 * dim]
    def final(i, carry):
        dshift, dscale = carry
        rows = pl.ds(pl.multiple_of(i * 16, 16), 16)
        nh, rstd = layer_norm_rows(x[rows, :].astype(F32))
        dh = rs.own(rows).astype(BF16).astype(F32)
        dn = dh * scale1
        prod = dh * nh
        dx = rstd * (dn - jnp.mean(dn, axis=-1, keepdims=True) - nh * jnp.mean(dn * nh, axis=-1, keepdims=True))
        g_new[rows, :] = (grad[rows, :].astype(F32) + dx).astype(BF16)
        return dshift + dh[:8] + dh[8:], dscale + prod[:8] + prod[8:]
    zero = jnp.zeros((8, dim), F32)
    dshift, dscale = lax.fori_loop(0, tok // 16, final, (zero, zero))
    d_shift[...] = jnp.sum(dshift, axis=0, keepdims=True)
    d_scale[...] = jnp.sum(dscale, axis=0, keepdims=True)
    rs.finish()


def bwd_in(blk, grad, x, mod, dproj, w):
    tok, dim = x.shape
    s = jax.ShapeDtypeStruct
    return pl.pallas_call(
        functools.partial(bwd_in_kernel, blk),
        out_shape=[s((tok, dim), BF16), s((1, dim), F32), s((1, dim), F32)],
        in_specs=[VM] * 3 + [ANY] * 2,
        out_specs=[VM] * 3,
        scratch_shapes=[pltpu.VMEM(w.shape, BF16), pltpu.VMEM(dproj.shape, BF16), pltpu.SemaphoreType.DMA,
                        pltpu.SemaphoreType.DMA((8,))] + reduce_scratch(tok, dim),
        compiler_params=comm_params(7 + blk),
        name=f"bwd_in{blk}",
    )(grad, x, mod, dproj, w)


def grad_win_kernel(h, dproj, *rest):
    out, stage = rest[-2], rest[-1]
    seq, tile = h.shape
    cols = dproj.shape[1] // 2
    row = lax.broadcasted_iota(jnp.int32, (256, 256), 0)
    lane = lax.broadcasted_iota(jnp.int32, (256, 256), 1)
    join = jnp.where(row == 2 * lax.rem(lane, 128) + lax.div(lane, 128), 1.0, 0.0).astype(BF16)
    stage[...] = dot(h[...], dproj[...], ((0,), (0,))).astype(BF16)
    for t in range(tile // 128):
        rows = slice(t * 128, (t + 1) * 128)
        both = jnp.concatenate([stage[rows, :cols], stage[rows, cols:]], axis=0)
        mixed = dot(join, both).astype(BF16)
        out[0, pl.ds(t * 128, 128)] = mixed.reshape(128, 2, cols)


def grad_win(blk, h, dproj, prev):
    seq = h.shape[0] * h.shape[1]
    dim = h.shape[2]
    width = dproj.shape[2]
    cols = width // 2
    tile = 256
    h2, dp2 = h.reshape(seq, dim), dproj.reshape(seq, width)
    args = [h2, dp2] + ([] if prev is None else [prev])
    return pl.pallas_call(
        grad_win_kernel,
        grid=(dim // tile,),
        out_shape=jax.ShapeDtypeStruct((2, dim, 2, cols), BF16),
        in_specs=[pl.BlockSpec((seq, tile), lambda i: (0, i)), VM] + ([] if prev is None else [ANY]),
        out_specs=pl.BlockSpec((1, tile, 2, cols), lambda i: (blk, i, 0, 0)),
        scratch_shapes=[pltpu.VMEM((tile, width), BF16)],
        input_output_aliases={} if prev is None else {2: 0},
        compiler_params=pltpu.CompilerParams(vmem_limit_bytes=VMEM_LIMIT),
        cost_estimate=pl.CostEstimate(flops=2 * seq * dim * width, bytes_accessed=2 * (seq * (dim + width) + dim * width), transcendentals=0),
        name=f"grad_win{blk}",
    )(*args)


def grad_wout_kernel(o, m, db, *rest):
    out = rest[-1]
    hd = o.shape[1] // 2
    mlp = m.shape[1] // 2
    for head in range(2):
        out[0, head, :hd, :] = dot(o[:, head * hd:(head + 1) * hd], db[...], ((0,), (0,))).astype(BF16)
        out[0, head, hd:, :] = dot(m[:, head * mlp:(head + 1) * mlp], db[...], ((0,), (0,))).astype(BF16)


def grad_wout(blk, o, m, db, prev):
    seq = o.shape[0] * o.shape[1]
    dim = db.shape[2]
    hd, mlp = o.shape[2] // 2, m.shape[2] // 2
    tile = min(256, dim)
    args = [o.reshape(seq, 2 * hd), m.reshape(seq, 2 * mlp), db.reshape(seq, dim)] + ([] if prev is None else [prev])
    return pl.pallas_call(
        grad_wout_kernel,
        grid=(dim // tile,),
        out_shape=jax.ShapeDtypeStruct((2, 2, hd + mlp, dim), BF16),
        in_specs=[VM, VM, pl.BlockSpec((seq, tile), lambda i: (0, i))] + ([] if prev is None else [ANY]),
        out_specs=pl.BlockSpec((1, 2, hd + mlp, tile), lambda i: (blk, 0, 0, i)),
        input_output_aliases={} if prev is None else {3: 0},
        compiler_params=pltpu.CompilerParams(vmem_limit_bytes=VMEM_LIMIT),
        cost_estimate=pl.CostEstimate(flops=4 * seq * dim * (hd + mlp), bytes_accessed=2 * seq * (dim + 2 * hd + 2 * mlp), transcendentals=0),
        name=f"grad_wout{blk}",
    )(*args)


def small_sum_kernel(vec, out, buf, gs, gr):
    nbrs = neighbours()
    buf[0] = vec[...]
    barrier(nbrs)
    gather = Gather(buf, gs, gr, nbrs, 1)
    gather.all_now()
    me = lax.axis_index("tp")
    core, xbit, ybit = lax.rem(me, 2), lax.rem(lax.div(me, 2), 2), lax.div(me, 4)
    total = None
    for owner in range(8):
        oc, ox, oy = owner % 2, (owner // 2) % 2, owner // 4
        slot = (core + oc - 2 * core * oc) + 2 * (xbit + ox - 2 * xbit * ox) + 4 * (ybit + oy - 2 * ybit * oy)
        total = buf[slot] if total is None else total + buf[slot]
    out[...] = total
    gather.finish()


def small_sum(vec):
    return pl.pallas_call(
        small_sum_kernel,
        out_shape=jax.ShapeDtypeStruct(vec.shape, F32),
        in_specs=[VM],
        out_specs=VM,
        scratch_shapes=[pltpu.VMEM((8,) + vec.shape, F32)] + gather_sems(1),
        compiler_params=comm_params(9),
        name="small_sum",
    )(vec)


def solution(mesh):
    act = P("dp", "tp", None)
    in_specs = (act, P("dp", None), P("tp", None), P("tp", None), P(None, None, None), P(None, None), P(None, None, "tp", None), P(None, "tp", None), P(None, None), P(None, None), P(None, "tp", None, None), P(None, None), act)
    out_specs = (act, act, P("dp", None, None), P("dp", None), P("dp", None, "tp", None), P("dp", "tp", None), P("dp", None), P("dp", None), P("dp", "tp", None, None), P("dp", None))

    def device_fn(x_in, cond_vec, rope_cos, rope_sin, w_mod, b_mod, w_in, b_in, q_scale, k_scale, w_out, b_out, d_out):
        blocks = w_in.shape[0]
        dim = x_in.shape[2]
        hd = q_scale.shape[1]
        mod, cosx, sinx = prologue(cond_vec, rope_cos, rope_sin, b_mod, w_mod)
        x = x_in[0]
        saved = []
        for blk in range(blocks):
            h, q, k, v, pre, u, m, w = fwd_in(blk, x, mod, b_in, q_scale, k_scale, cosx, sinx, w_in)
            x_new, branch, o, of, lse = fwd_out(blk, x, mod, b_out, k, v, q, m, w_out)
            saved.append((x, h, q, k, v, pre, u, m, w, branch, o, of, lse))
            x = x_new
        grad = d_out[0]
        gwin = gwout = None
        small, gbin = {}, {}
        for blk in reversed(range(blocks)):
            xb, h, q, k, v, pre, u, m, w, branch, o, of, lse = saved[blk]
            db, dproj, gb, d_gate, d_bout, d_qs, d_ks = bwd_out(blk, grad, branch, mod, q_scale, k_scale, k, v, q, cosx, sinx, of, lse, pre, u, w_out)
            grad, d_shift, d_scale = bwd_in(blk, grad, xb, mod, dproj, w)
            gwin = grad_win(blk, h, dproj, gwin)
            gwout = grad_wout(blk, o, m, db, gwout)
            small[blk] = jnp.concatenate([d_shift, d_scale, d_gate, d_bout, d_qs, d_ks], axis=1)
            gbin[blk] = gb
        sums = small_sum(jnp.concatenate([small[blk] for blk in range(blocks)], axis=0))
        d_mod = sums[:, :3 * dim]
        vec = cond_vec.astype(F32)
        silu = jax.nn.silu(vec).astype(BF16).astype(F32)
        g_wmod = silu[0][None, :, None] * d_mod[:, None, :]
        g_bin = jnp.stack([gbin[blk].reshape(2, -1) for blk in range(blocks)])
        return (x[None], grad[None], g_wmod, d_mod, gwin, g_bin, sums[:, 4 * dim:4 * dim + hd], sums[:, 4 * dim + hd:],
                gwout, sums[:, 3 * dim:4 * dim])

    return jax.shard_map(device_fn, mesh=mesh, in_specs=in_specs, out_specs=out_specs, check_vma=False)
```
